32 devices in a mesh: rep: 2 (over x), dp: 16 (over y, z, core).
Axes of the slice: x: 2, y: 2, z: 4, core: 2. Of those that a mesh axis runs over, the one named last changes fastest.
Arguments:
- g_w_gate: bfloat16 [32, 2, 896, 2560], P(('rep', 'dp')), parts along dimension 0
- g_w_up: bfloat16 [32, 2, 896, 2560], P(('rep', 'dp')), parts along dimension 0
- g_w_down: bfloat16 [32, 2, 2560, 896], P(('rep', 'dp')), parts along dimension 0
- w_gate: bfloat16 [2, 896, 2560], replicated
- w_up: bfloat16 [2, 896, 2560], replicated
- w_down: bfloat16 [2, 2560, 896], replicated
- m_w_gate: float32 [2, 896, 2560], P(None, 'dp')
- m_w_up: float32 [2, 896, 2560], P(None, 'dp')
- m_w_down: float32 [2, 2560, 896], P(None, 'dp')
- v_w_gate: float32 [2, 896, 2560], P(None, 'dp')
- v_w_up: float32 [2, 896, 2560], P(None, 'dp')
- v_w_down: float32 [2, 2560, 896], P(None, 'dp')
Outputs:
- output 1: bfloat16 [4, 896, 2560], P('rep'), parts along dimension 0
- output 2: bfloat16 [4, 896, 2560], P('rep'), parts along dimension 0
- output 3: bfloat16 [4, 2560, 896], P('rep'), parts along dimension 0
- output 4: float32 [4, 896, 2560], P('rep', 'dp'), parts along dimension 0
- output 5: float32 [4, 896, 2560], P('rep', 'dp'), parts along dimension 0
- output 6: float32 [4, 2560, 896], P('rep', 'dp'), parts along dimension 0
- output 7: float32 [4, 896, 2560], P('rep', 'dp'), parts along dimension 0
- output 8: float32 [4, 896, 2560], P('rep', 'dp'), parts along dimension 0
- output 9: float32 [4, 2560, 896], P('rep', 'dp'), parts along dimension 0
There are 2 independent parts. The reference program is written for one: setup_inputs(seed, part) draws one part's arguments, and reference() takes and returns one part's arrays. A program takes and returns all parts, laid end to end along the dimension named above; an argument that names none is the same for every part.
All inputs are finite; a program needn't handle non-finite values.
Results may differ from the reference program's by a relative error of at most 0.022.
Values are sent between devices in bfloat16 or wider.
A program may use at most 2 GiB of HBM per device.

```python
import jax
import jax.numpy as jnp
from jax import lax

DEVICES = 16
D = 896
FF = 2560
LAYERS = 2
NAMES = ("w_gate", "w_up", "w_down")
SHAPES = {"w_gate": (LAYERS, D, FF), "w_up": (LAYERS, D, FF), "w_down": (LAYERS, FF, D)}


def setup_inputs(seed: int = 0, part: int = 0) -> dict:
    kz, *keys = jax.random.split(jax.random.key(seed), 1 + 5 * len(NAMES))
    loud = 2.0 ** jax.random.uniform(kz, (), jnp.float32, -1.0, 1.0)
    drawn = {}
    for name, key, both in zip(NAMES, keys[:3], keys[3:6], strict=True):
        own = jax.random.normal(jax.random.fold_in(key, part), (DEVICES, *SHAPES[name]), jnp.float32)
        shared = jax.random.normal(jax.random.fold_in(both, part), SHAPES[name], jnp.float32)
        drawn["g_" + name] = (loud * (0.7 * shared / DEVICES + 0.7 * own * DEVICES**-0.5)).astype(jnp.bfloat16)
    for name, key in zip(NAMES, keys[6:9], strict=True):
        drawn[name] = (jax.random.normal(key, SHAPES[name], jnp.float32) * SHAPES[name][1] ** -0.5).astype(jnp.bfloat16)
    for name, key in zip(NAMES, keys[9:12], strict=True):
        drawn["m_" + name] = loud * 0.5 * jax.random.normal(key, SHAPES[name], jnp.float32)
    for name, key in zip(NAMES, keys[12:15], strict=True):
        drawn["v_" + name] = loud * loud * jax.random.uniform(key, SHAPES[name], jnp.float32, 0.5, 1.5)
    return drawn


def adamw(w, m, v, g):
    m = 0.9 * m + 0.1 * g
    v = 0.95 * v + 0.05 * g * g
    step = m * lax.rsqrt(v + 1e-8) + 0.1 * w
    return (w - 0.02 * step).astype(jnp.bfloat16), m, v


def clipped(gradients, sum_of_squares, count):
    factor = jnp.minimum(1.0, 0.5 * lax.rsqrt(sum_of_squares / count + 1e-30))
    return [g * factor for g in gradients]


def reference(g_w_gate, g_w_up, g_w_down, w_gate, w_up, w_down, m_w_gate, m_w_up, m_w_down, v_w_gate, v_w_up, v_w_down):
    def total(terms):
        return lax.scan(lambda so_far, term: (so_far + term.astype(jnp.float32), None), jnp.zeros(terms.shape[1:], jnp.float32), terms)[0]

    gradients = [total(terms).astype(jnp.bfloat16).astype(jnp.float32) for terms in (g_w_gate, g_w_up, g_w_down)]
    gradients = clipped(gradients, sum(jnp.sum(g * g) for g in gradients), sum(g.size for g in gradients))
    new = [
        adamw(w.astype(jnp.float32), m, v, g)
        for w, m, v, g in zip((w_gate, w_up, w_down), (m_w_gate, m_w_up, m_w_down), (v_w_gate, v_w_up, v_w_down), gradients, strict=True)
    ]
    return tuple(one[which] for which in range(3) for one in new)
```

```python
import jax
import jax.numpy as jnp
from jax import lax
from jax.experimental import pallas as pl
from jax.experimental.pallas import tpu as pltpu
from jax.sharding import PartitionSpec as P

F32, BF16 = jnp.float32, jnp.bfloat16
NY, NZ, NC = 2, 4, 2
L, D, FF = 2, 896, 2560
RA, RB = D // 16, FF // 16
CA, HB = FF // 2, RB // 2
COUNT = 3 * L * D * FF


class Sub:
    def __init__(self, k, kind, m, l, h, i, two):
        self.k, self.kind, self.m, self.l, self.h, self.i, self.two = k, kind, m, l, h, i, two

    @property
    def cols(self):
        return pl.ds(self.h * CA, CA)

    @property
    def rows(self):
        return pl.ds(self.h * HB, HB)


def subunits():
    subs = []
    for m in range(2):
        for l in range(L):
            for h in range(2):
                subs.append(Sub(len(subs), "A", m, l, h, len(subs), False))
    for l in range(L):
        for h in range(2):
            subs.append(Sub(len(subs), "B", 0, l, h, l * 2 + h, l == 1))
    return subs


SUBS = subunits()
FIRST_Y = [s for s in SUBS if not s.two]
FIRST_Z = [s for s in SUBS if s.two]
NS = len(SUBS)
STEPS = 5


def tile(sub, j):
    if sub.kind == "A":
        return (slice(None), pl.ds(pl.multiple_of(j * 256, 256), 256))
    return (pl.ds(pl.multiple_of(j * 16, 16), 16), slice(None))


def body(
    g_gate, g_up, g_down, w_gate, w_up, w_down, mg, mu, md, vg, vu, vd,
    WG, WU, WB, MA, MB, VA, VB,
    YA, YB, YC, ZA, ZB, ZC, GA, GB, OA, OB, NB,
    ld_sem, mv_sem, ds_sem, dr_sem, ys_sem, yr_sem, zs_sem, zr_sem, ns_sem, nr_sem,
):
    me = lax.axis_index("dp")
    c = me % 2
    z = (me // 2) % NZ
    y = me // (2 * NZ)
    side = z // 2
    r = jnp.where(side == 0, z, 3 - z)
    inner = r == 1
    away, toward = side, 1 - side

    def dev(yy, zz, cc):
        return {"dp": (yy * NZ + zz) * NC + cc}

    partner = dev(y, z, 1 - c)
    across = dev(1 - y, z, c)
    away_dev = dev(y, z + 1 - 2 * away, c)

    def z_dev(direction):
        return dev(y, z + 1 - 2 * direction, c)

    def absolute(t):
        return t + side * (3 - 2 * t)

    def slot(t, direction):
        return jnp.clip(t - 1 + direction, 0, 2)

    def W(s, yy, zz, cc):
        if s.kind == "A":
            return (WG, WU)[s.m].at[s.l, yy, zz, cc, :, s.cols]
        return WB.at[s.l, yy, zz, cc, s.rows, :]

    def G_in(s, cc):
        if s.kind == "A":
            return (g_gate, g_up)[s.m].at[s.l, :, :, cc, :, s.cols]
        return g_down.at[s.l, :, :, cc, s.rows, :]

    def Y(s, t):
        return YA.at[s.i, t] if s.kind == "A" else YB.at[s.i, t]

    def Z(s, direction, sl):
        return ZA.at[s.i, direction, sl] if s.kind == "A" else ZB.at[s.i, direction, sl]

    def Z2(s, direction, sl):
        return ZC.at[s.h, direction, sl]

    def G(s):
        return GA.at[s.i] if s.kind == "A" else GB.at[s.i]

    def state(s, A, B):
        return A.at[s.m, s.l, :, s.cols] if s.kind == "A" else B.at[s.l, s.rows, :]

    def remote(src, dst, ss, rs, device):
        return pltpu.make_async_remote_copy(src, dst, ss, rs, device_id=device, device_id_type=pl.DeviceIdType.MESH)

    def got(ref, sem):
        remote(ref, ref, sem, sem, partner).wait_recv()

    def sent(ref, sem):
        remote(ref, ref, sem, sem, partner).wait_send()

    barrier = pltpu.get_barrier_semaphore()
    others = [dev(y, (z + d) % NZ, c) for d in range(1, NZ)]
    for peer in (partner, across, *others):
        pl.semaphore_signal(barrier, inc=1, device_id=peer, device_id_type=pl.DeviceIdType.MESH)
    pl.semaphore_wait(barrier, 5)

    def load(s):
        return pltpu.make_async_copy(G_in(s, c), W(s, slice(None), slice(None), c), ld_sem.at[s.k])

    def half(s):
        return remote(G_in(s, 1 - c), W(s, slice(None), slice(None), c), ds_sem.at[s.k, 0], dr_sem.at[s.k, 0], partner)

    start_order = FIRST_Y[:2] + FIRST_Z + FIRST_Y[2:]
    for s in start_order:
        half(s).start()
        load(s).start()
    chip = (y, z)
    extra = []
    for n, (src, A) in enumerate(((w_gate, OA), (w_up, OA))):
        extra.append(pltpu.make_async_copy(src.at[:, y, z, c], A.at[n], mv_sem.at[n]))
    extra.append(pltpu.make_async_copy(w_down.at[:, y, z, c], OB, mv_sem.at[2]))
    for n, (src, dst) in enumerate(((mg, MA.at[0]), (mu, MA.at[1]), (md, MB), (vg, VA.at[0]), (vu, VA.at[1]), (vd, VB))):
        extra.append(pltpu.make_async_copy(src, dst, mv_sem.at[3 + n]))
    for copy in extra:
        copy.start()

    def ready(s):
        load(s).wait()
        got(W(s, slice(None), slice(None), 1 - c), dr_sem.at[s.k, 0])

    def total(s, srcs, maybe):
        def at(ix):
            out = None
            for ref in srcs:
                one = ref[ix].astype(F32)
                out = one if out is None else out + one
            for ref in maybe:
                out = out + jnp.where(inner, ref[ix].astype(F32), 0.0)
            return out

        return at

    def add_into(s, dst, srcs, maybe=()):
        value = total(s, srcs, maybe)

        def one(j, carry):
            ix = tile(s, j)
            dst[ix] = value(ix).astype(BF16)
            return carry

        lax.fori_loop(0, STEPS, one, 0)

    def finish(s, acc, srcs, maybe=()):
        value = total(s, srcs, maybe)

        def one(j, carry):
            ix = tile(s, j)
            g = value(ix).astype(BF16)
            G(s)[ix] = g
            g = g.astype(F32)
            g = g * g
            for a in range(g.shape[0] // 8):
                for b in range(g.shape[1] // 128):
                    carry = carry + g[a * 8 : a * 8 + 8, b * 128 : b * 128 + 128]
            return carry

        return lax.fori_loop(0, STEPS, one, acc)

    steps = [(3, away), (2, away), (1 - r, jnp.where(inner, toward, away))]
    y_order = [3, 2, 1 - r, r]

    def y_copy(s, q):
        t = absolute(y_order[q])
        return remote(W(s, 1 - y, t, 1 - c), Y(s, t), ys_sem.at[s.k, q], yr_sem.at[s.k, q], across)

    def y_send(s):
        ready(s)
        for q in range(4):
            t = absolute(y_order[q])
            dst = W(s, 1 - y, t, 1 - c)
            add_into(s, dst, [W(s, 1 - y, t, c), dst])
            y_copy(s, q).start()

    def z_copy(s, q):
        t, direction = absolute(steps[q][0]), steps[q][1]
        sl = slot(t, direction)
        ref = Z(s, direction, sl) if not s.two else Z2(s, direction, sl)
        return remote(ref, ref, zs_sem.at[s.k, q], zr_sem.at[s.k, direction * 3 + sl], z_dev(direction)), ref, sl, t, direction

    def chain(s):
        for q in range(3):
            copy, ref, sl, t, direction = z_copy(s, q)
            got(Y(s, t), yr_sem.at[s.k, q])

            @pl.when(inner)
            def _():
                got(ref, zr_sem.at[s.k, direction * 3 + sl])

            add_into(s, ref, [W(s, y, t, c), W(s, y, t, 1 - c), Y(s, t)], [ref])
            copy.start()

    def chain_end(s, acc):
        t = absolute(r)
        got(Y(s, t), yr_sem.at[s.k, 3])
        view = Z if not s.two else Z2
        near, far = slot(t, away), slot(t, toward)
        got(view(s, toward, far), zr_sem.at[s.k, toward * 3 + far])

        @pl.when(inner)
        def _():
            got(view(s, away, near), zr_sem.at[s.k, away * 3 + near])

        return finish(s, acc, [W(s, y, t, c), W(s, y, t, 1 - c), Y(s, t), view(s, toward, far)], [view(s, away, near)])

    def chain2(s):
        ready(s)
        for q in range(3):
            copy, ref, sl, t, direction = z_copy(s, q)

            @pl.when(inner)
            def _():
                got(ref, zr_sem.at[s.k, direction * 3 + sl])

            for yy in range(2):
                add_into(s, ref.at[yy], [W(s, yy, t, c), W(s, yy, t, 1 - c)], [ref.at[yy]])
            copy.start()

    def ends2(s):
        t = absolute(r)
        return t, Z2(s, toward, slot(t, toward)), Z2(s, away, slot(t, away))

    def y_copy2(s):
        t, far, near = ends2(s)
        return remote(far.at[1 - y], YC.at[s.h], ys_sem.at[s.k, 0], yr_sem.at[s.k, 0], across)

    def y_send2(s):
        t, far, near = ends2(s)
        got(far, zr_sem.at[s.k, toward * 3 + slot(t, toward)])

        @pl.when(inner)
        def _():
            got(near, zr_sem.at[s.k, away * 3 + slot(t, away)])

        dst = far.at[1 - y]
        add_into(s, dst, [W(s, 1 - y, t, c), W(s, 1 - y, t, 1 - c), dst], [near.at[1 - y]])
        y_copy2(s).start()

    def end2(s, acc):
        t, far, near = ends2(s)
        got(YC.at[s.h], yr_sem.at[s.k, 0])
        return finish(s, acc, [W(s, y, t, c), W(s, y, t, 1 - c), far.at[y], YC.at[s.h]], [near.at[y]])

    ahead = 4
    for s in FIRST_Y[:ahead]:
        y_send(s)
    for s in FIRST_Z:
        chain2(s)
    for s in FIRST_Z:
        y_send2(s)
    acc = jnp.zeros((8, 128), F32)
    for n, s in enumerate(FIRST_Y):
        if n + ahead < len(FIRST_Y):
            y_send(FIRST_Y[n + ahead])
        chain(s)
        acc = chain_end(s, acc)
    for s in FIRST_Z:
        acc = end2(s, acc)

    for s in SUBS:
        half(s).wait_send()
        for q in range(3):
            z_copy(s, q)[0].wait_send()
        if s.two:
            y_copy2(s).wait_send()
        else:
            for q in range(4):
                y_copy(s, q).wait_send()
    for copy in extra:
        copy.wait()

    NB[0] = acc
    copy = remote(NB.at[0], NB.at[1], ns_sem.at[0], nr_sem.at[0], partner)
    copy.start()
    copy.wait()
    NB[2] = NB[0] + NB[1]
    copy = remote(NB.at[2], NB.at[3], ns_sem.at[1], nr_sem.at[1], across)
    copy.start()
    copy.wait()
    NB[4] = NB[2] + NB[3]
    copies = [remote(NB.at[4], NB.at[4 + d], ns_sem.at[1 + d], nr_sem.at[1 + d], others[d - 1]) for d in range(1, NZ)]
    for copy in copies:
        copy.start()
    for copy in copies:
        copy.wait()
    squares = jnp.sum(NB[4] + NB[5] + NB[6] + NB[7], keepdims=True)
    factor = jnp.minimum(1.0, 0.5 * lax.rsqrt(squares / COUNT + 1e-30))

    def adamw(s):
        m_ref, v_ref, w_ref, out = state(s, MA, MB), state(s, VA, VB), state(s, OA, OB), W(s, y, z, c)

        def one(j, carry):
            ix = tile(s, j)
            g = G(s)[ix].astype(F32) * factor
            m = 0.9 * m_ref[ix] + 0.1 * g
            v = 0.95 * v_ref[ix] + 0.05 * g * g
            w = w_ref[ix].astype(F32)
            m_ref[ix] = m
            v_ref[ix] = v
            out[ix] = (w - 0.02 * (m * lax.rsqrt(v + 1e-8) + 0.1 * w)).astype(BF16)
            return carry

        lax.fori_loop(0, STEPS, one, 0)

    def piece(s, t):
        return W(s, slice(None) if s.two else y, t, c)

    def z_go(s, n, t, direction):
        ref = piece(s, t)
        return remote(ref, ref, zs_sem.at[s.k, n], zr_sem.at[s.k, t], z_dev(direction))

    def y_go(s, n, t):
        ref = W(s, y, t, c)
        return remote(ref, ref, ys_sem.at[s.k, n], yr_sem.at[s.k, t], across)

    def core_go(s, n, yy):
        ref = W(s, yy, slice(None), c)
        return remote(ref, ref, ds_sem.at[s.k, n], dr_sem.at[s.k, n], partner)

    def z_own(s):
        z_go(s, 0, z, away).start()

        @pl.when(inner)
        def _():
            z_go(s, 1, z, toward).start()

    events = [(1 - r, away), (2, toward), (3, toward)]

    def z_events(s):
        for e, (t, direction) in enumerate(events):
            t = absolute(t)
            got(piece(s, t), zr_sem.at[s.k, t])

            @pl.when(inner)
            def _():
                z_go(s, 2 + e, t, direction).start()

            if not s.two:
                y_go(s, 1 + e, t).start()
        if s.two:
            core_go(s, 0, slice(None)).start()
        else:
            core_go(s, 0, y).start()

    def y_end(s):
        for t in range(NZ):
            got(W(s, 1 - y, t, c), yr_sem.at[s.k, t])
        core_go(s, 1, 1 - y).start()

    def own(s):
        adamw(s)
        if s.two:
            y_go(s, 0, z).start()
        else:
            z_own(s)
            y_go(s, 0, z).start()

    def own2(s):
        got(W(s, 1 - y, z, c), yr_sem.at[s.k, z])
        z_own(s)

    own(FIRST_Y[0])
    for s in FIRST_Z:
        own(s)
    own(FIRST_Y[1])
    ended = 0
    for n, s in enumerate(FIRST_Y):
        if n + 2 < len(FIRST_Y):
            own(FIRST_Y[n + 2])
        if n + 2 == len(FIRST_Y):
            own2(FIRST_Z[0])
        if n + 1 == len(FIRST_Y):
            own2(FIRST_Z[1])
        z_events(s)
        if ended + 1 <= (2 * n) // 3 - 1:
            y_end(FIRST_Y[ended])
            ended += 1
    for s in FIRST_Z:
        y_end(FIRST_Y[ended])
        ended += 1
        z_events(s)
    while ended < len(FIRST_Y):
        y_end(FIRST_Y[ended])
        ended += 1

    for s in SUBS:
        if s.two:
            got(W(s, slice(None), slice(None), 1 - c), dr_sem.at[s.k, 0])
            core_go(s, 0, slice(None)).wait_send()
            y_go(s, 0, z).wait_send()
        else:
            got(W(s, y, slice(None), 1 - c), dr_sem.at[s.k, 0])
            got(W(s, 1 - y, slice(None), 1 - c), dr_sem.at[s.k, 1])
            core_go(s, 0, y).wait_send()
            core_go(s, 1, 1 - y).wait_send()
            for n in range(4):
                y_go(s, n, z).wait_send()
        z_go(s, 0, z, away).wait_send()

        @pl.when(inner)
        def _():
            for n in range(1, 5):
                z_go(s, n, z, away).wait_send()


def write_out(WG, WU, WB, MA, MB, VA, VB, *refs):
    outs, sem = refs[:9], refs[9]
    copies = []
    for src, dst in ((WG, outs[0]), (WU, outs[1]), (WB, outs[2])):
        for l in range(L):
            copies += [(src.at[l, yy], dst.at[l, yy]) for yy in range(NY)]
    for A, B, first in ((MA, MB, 3), (VA, VB, 6)):
        copies += [(A.at[0], outs[first]), (A.at[1], outs[first + 1]), (B, outs[first + 2])]
    copies = [pltpu.make_async_copy(src, dst, sem.at[n]) for n, (src, dst) in enumerate(copies)]
    for copy in copies:
        copy.start()
    for copy in copies:
        copy.wait()


def solution(mesh):
    nh = len([s for s in FIRST_Y if s.kind == "B"])
    hbm = pl.BlockSpec(memory_space=pltpu.MemorySpace.HBM)
    vmem = pl.BlockSpec(memory_space=pltpu.MemorySpace.VMEM)
    held = [
        ((L, NY, NZ, NC, RA, FF), BF16),
        ((L, NY, NZ, NC, RA, FF), BF16),
        ((L, NY, NZ, NC, RB, D), BF16),
        ((2, L, RA, FF), F32),
        ((L, RB, D), F32),
        ((2, L, RA, FF), F32),
        ((L, RB, D), F32),
    ]

    def step(*arrays):
        terms, weights, m, v = (arrays[i : i + 3] for i in (0, 3, 6, 9))

        def split(x):
            rows = x.shape[-2] // 16
            return x.reshape(L, NY, NZ, NC, rows, x.shape[-1])

        kept = pl.pallas_call(
            body,
            name="step",
            out_shape=[pltpu.VMEM(shape, dtype) for shape, dtype in held],
            in_specs=[hbm] * 12,
            out_specs=[vmem] * 7,
            scratch_shapes=[
                pltpu.VMEM((8, NZ, RA, CA), BF16),
                pltpu.VMEM((nh, NZ, HB, D), BF16),
                pltpu.VMEM((2, HB, D), BF16),
                pltpu.VMEM((8, 2, 3, RA, CA), BF16),
                pltpu.VMEM((nh, 2, 3, HB, D), BF16),
                pltpu.VMEM((2, 2, 3, NY, HB, D), BF16),
                pltpu.VMEM((8, RA, CA), BF16),
                pltpu.VMEM((4, HB, D), BF16),
                pltpu.VMEM((2, L, RA, FF), BF16),
                pltpu.VMEM((L, RB, D), BF16),
                pltpu.VMEM((8, 8, 128), F32),
                pltpu.SemaphoreType.DMA((NS,)),
                pltpu.SemaphoreType.DMA((9,)),
                pltpu.SemaphoreType.DMA((NS, 2)),
                pltpu.SemaphoreType.DMA((NS, 2)),
                pltpu.SemaphoreType.DMA((NS, 4)),
                pltpu.SemaphoreType.DMA((NS, 4)),
                pltpu.SemaphoreType.DMA((NS, 5)),
                pltpu.SemaphoreType.DMA((NS, 6)),
                pltpu.SemaphoreType.DMA((5,)),
                pltpu.SemaphoreType.DMA((5,)),
            ],
            compiler_params=pltpu.CompilerParams(collective_id=0, has_side_effects=True, vmem_limit_bytes=28 * 2**20),
        )(*(split(t[0]) for t in terms), *(split(w) for w in weights), *m, *v)

        outs = pl.pallas_call(
            write_out,
            name="write_out",
            out_shape=[jax.ShapeDtypeStruct((L, NY, NZ, NC, RA, FF), BF16)] * 2
            + [jax.ShapeDtypeStruct((L, NY, NZ, NC, RB, D), BF16)]
            + ([jax.ShapeDtypeStruct((L, RA, FF), F32)] * 2 + [jax.ShapeDtypeStruct((L, RB, D), F32)]) * 2,
            in_specs=[vmem] * 7,
            out_specs=[hbm] * 9,
            scratch_shapes=[pltpu.SemaphoreType.DMA((18,))],
            compiler_params=pltpu.CompilerParams(vmem_limit_bytes=2 * 2**20),
        )(*kept)
        whole = [x.reshape(L, -1, x.shape[-1]) for x in outs[:3]]
        return (*whole, *outs[3:])

    all_of, cut = P(None, None, None), P(None, "dp", None)
    return jax.shard_map(
        step,
        mesh=mesh,
        in_specs=(P(("rep", "dp"), None, None, None),) * 3 + (all_of,) * 3 + (cut,) * 6,
        out_specs=(P("rep", None, None),) * 3 + (P("rep", "dp", None),) * 6,
        check_vma=False,
    )
```

```python
import jax
import jax.numpy as jnp
from jax import lax
from jax.experimental import pallas as pl
from jax.experimental.pallas import tpu as pltpu
from jax.sharding import PartitionSpec as P

F32, BF16 = jnp.float32, jnp.bfloat16
NY, NZ, NC = 2, 4, 2
L, D, FF = 2, 896, 2560
RA, RB = D // 16, FF // 16
CA, HB = FF // 2, RB // 2
COUNT = 3 * L * D * FF


class Sub:
    def __init__(self, k, kind, m, l, h, i, two):
        self.k, self.kind, self.m, self.l, self.h, self.i, self.two = k, kind, m, l, h, i, two

    @property
    def cols(self):
        return pl.ds(self.h * CA, CA)

    @property
    def rows(self):
        return pl.ds(self.h * HB, HB)


def subunits():
    subs = []
    for m in range(2):
        for l in range(L):
            for h in range(2):
                subs.append(Sub(len(subs), "A", m, l, h, len(subs), False))
    for l in range(L):
        for h in range(2):
            subs.append(Sub(len(subs), "B", 0, l, h, l * 2 + h, l == 1))
    return subs


SUBS = subunits()
FIRST_Y = [s for s in SUBS if not s.two]
FIRST_Z = [s for s in SUBS if s.two]
NS = len(SUBS)
STEPS = 5


def tile(sub, j):
    if sub.kind == "A":
        return (slice(None), pl.ds(pl.multiple_of(j * 256, 256), 256))
    return (pl.ds(pl.multiple_of(j * 16, 16), 16), slice(None))


def body(
    g_gate, g_up, g_down, w_gate, w_up, w_down, mg, mu, md, vg, vu, vd,
    WG, WU, WB, MA, MB, VA, VB,
    YA, YB, YC, ZA, ZB, ZC, GA, GB, OA, OB, NB,
    ld_sem, mv_sem, ds_sem, dr_sem, ys_sem, yr_sem, zs_sem, zr_sem, ns_sem, nr_sem,
):
    me = lax.axis_index("dp")
    c = me % 2
    z = (me // 2) % NZ
    y = me // (2 * NZ)
    side = z // 2
    r = jnp.where(side == 0, z, 3 - z)
    inner = r == 1
    away, toward = side, 1 - side

    def dev(yy, zz, cc):
        return {"dp": (yy * NZ + zz) * NC + cc}

    partner = dev(y, z, 1 - c)
    across = dev(1 - y, z, c)
    away_dev = dev(y, z + 1 - 2 * away, c)

    def z_dev(direction):
        return dev(y, z + 1 - 2 * direction, c)

    def absolute(t):
        return t + side * (3 - 2 * t)

    def slot(t, direction):
        return jnp.clip(t - 1 + direction, 0, 2)

    def W(s, yy, zz, cc):
        if s.kind == "A":
            return (WG, WU)[s.m].at[s.l, yy, zz, cc, :, s.cols]
        return WB.at[s.l, yy, zz, cc, s.rows, :]

    def G_in(s, cc):
        if s.kind == "A":
            return (g_gate, g_up)[s.m].at[s.l, :, :, cc, :, s.cols]
        return g_down.at[s.l, :, :, cc, s.rows, :]

    def Y(s, t):
        return YA.at[s.i, t] if s.kind == "A" else YB.at[s.i, t]

    def Z(s, direction, sl):
        return ZA.at[s.i, direction, sl] if s.kind == "A" else ZB.at[s.i, direction, sl]

    def Z2(s, direction, sl):
        return ZC.at[s.h, direction, sl]

    def G(s):
        return GA.at[s.i] if s.kind == "A" else GB.at[s.i]

    def state(s, A, B):
        return A.at[s.m, s.l, :, s.cols] if s.kind == "A" else B.at[s.l, s.rows, :]

    def remote(src, dst, ss, rs, device):
        return pltpu.make_async_remote_copy(src, dst, ss, rs, device_id=device, device_id_type=pl.DeviceIdType.MESH)

    def got(ref, sem):
        remote(ref, ref, sem, sem, partner).wait_recv()

    def sent(ref, sem):
        remote(ref, ref, sem, sem, partner).wait_send()

    barrier = pltpu.get_barrier_semaphore()
    others = [dev(y, (z + d) % NZ, c) for d in range(1, NZ)]
    for peer in (partner, across, *others):
        pl.semaphore_signal(barrier, inc=1, device_id=peer, device_id_type=pl.DeviceIdType.MESH)
    pl.semaphore_wait(barrier, 5)

    def load(s):
        return pltpu.make_async_copy(G_in(s, c), W(s, slice(None), slice(None), c), ld_sem.at[s.k])

    def half(s):
        return remote(G_in(s, 1 - c), W(s, slice(None), slice(None), c), ds_sem.at[s.k, 0], dr_sem.at[s.k, 0], partner)

    start_order = FIRST_Y[:2] + FIRST_Z[:1] + FIRST_Y[2:4] + FIRST_Z[1:] + FIRST_Y[4:]
    for s in start_order:
        half(s).start()
        load(s).start()
    chip = (y, z)
    extra = []
    for n, (src, A) in enumerate(((w_gate, OA), (w_up, OA))):
        extra.append(pltpu.make_async_copy(src.at[:, y, z, c], A.at[n], mv_sem.at[n]))
    extra.append(pltpu.make_async_copy(w_down.at[:, y, z, c], OB, mv_sem.at[2]))
    for n, (src, dst) in enumerate(((mg, MA.at[0]), (mu, MA.at[1]), (md, MB), (vg, VA.at[0]), (vu, VA.at[1]), (vd, VB))):
        extra.append(pltpu.make_async_copy(src, dst, mv_sem.at[3 + n]))
    for copy in extra:
        copy.start()

    def ready(s):
        load(s).wait()
        got(W(s, slice(None), slice(None), 1 - c), dr_sem.at[s.k, 0])

    def total(s, srcs, maybe):
        def at(ix):
            out = None
            for ref in srcs:
                one = ref[ix].astype(F32)
                out = one if out is None else out + one
            for ref in maybe:
                out = out + jnp.where(inner, ref[ix].astype(F32), 0.0)
            return out

        return at

    def add_into(s, dst, srcs, maybe=()):
        value = total(s, srcs, maybe)

        def one(j, carry):
            ix = tile(s, j)
            dst[ix] = value(ix).astype(BF16)
            return carry

        lax.fori_loop(0, STEPS, one, 0)

    def finish(s, acc, srcs, maybe=()):
        value = total(s, srcs, maybe)

        def one(j, carry):
            ix = tile(s, j)
            g = value(ix).astype(BF16)
            G(s)[ix] = g
            g = g.astype(F32)
            g = g * g
            for a in range(g.shape[0] // 8):
                for b in range(g.shape[1] // 128):
                    carry = carry + g[a * 8 : a * 8 + 8, b * 128 : b * 128 + 128]
            return carry

        return lax.fori_loop(0, STEPS, one, acc)

    steps = [(3, away), (2, away), (1 - r, jnp.where(inner, toward, away))]
    y_order = [3, 2, 1 - r, r]

    def y_copy(s, q):
        t = absolute(y_order[q])
        return remote(W(s, 1 - y, t, 1 - c), Y(s, t), ys_sem.at[s.k, q], yr_sem.at[s.k, q], across)

    def y_send(s):
        ready(s)
        for q in range(4):
            t = absolute(y_order[q])
            dst = W(s, 1 - y, t, 1 - c)
            add_into(s, dst, [W(s, 1 - y, t, c), dst])
            y_copy(s, q).start()

    def z_copy(s, q):
        t, direction = absolute(steps[q][0]), steps[q][1]
        sl = slot(t, direction)
        ref = Z(s, direction, sl) if not s.two else Z2(s, direction, sl)
        return remote(ref, ref, zs_sem.at[s.k, q], zr_sem.at[s.k, direction * 3 + sl], z_dev(direction)), ref, sl, t, direction

    def chain(s, qs):
        for q in qs:
            copy, ref, sl, t, direction = z_copy(s, q)
            got(Y(s, t), yr_sem.at[s.k, q])

            @pl.when(inner)
            def _():
                got(ref, zr_sem.at[s.k, direction * 3 + sl])

            add_into(s, ref, [W(s, y, t, c), W(s, y, t, 1 - c), Y(s, t)], [ref])
            copy.start()

    def chain_end(s, acc):
        t = absolute(r)
        got(Y(s, t), yr_sem.at[s.k, 3])
        view = Z if not s.two else Z2
        near, far = slot(t, away), slot(t, toward)
        got(view(s, toward, far), zr_sem.at[s.k, toward * 3 + far])

        @pl.when(inner)
        def _():
            got(view(s, away, near), zr_sem.at[s.k, away * 3 + near])

        return finish(s, acc, [W(s, y, t, c), W(s, y, t, 1 - c), Y(s, t), view(s, toward, far)], [view(s, away, near)])

    def chain2(s, qs):
        for q in qs:
            copy, ref, sl, t, direction = z_copy(s, q)

            @pl.when(inner)
            def _():
                got(ref, zr_sem.at[s.k, direction * 3 + sl])

            for yy in range(2):
                add_into(s, ref.at[yy], [W(s, yy, t, c), W(s, yy, t, 1 - c)], [ref.at[yy]])
            copy.start()

    def ends2(s):
        t = absolute(r)
        return t, Z2(s, toward, slot(t, toward)), Z2(s, away, slot(t, away))

    def y_copy2(s):
        t, far, near = ends2(s)
        return remote(far.at[1 - y], YC.at[s.h], ys_sem.at[s.k, 0], yr_sem.at[s.k, 0], across)

    def y_send2(s):
        t, far, near = ends2(s)
        got(far, zr_sem.at[s.k, toward * 3 + slot(t, toward)])

        @pl.when(inner)
        def _():
            got(near, zr_sem.at[s.k, away * 3 + slot(t, away)])

        dst = far.at[1 - y]
        add_into(s, dst, [W(s, 1 - y, t, c), W(s, 1 - y, t, 1 - c), dst], [near.at[1 - y]])
        y_copy2(s).start()

    def end2(s, acc):
        t, far, near = ends2(s)
        got(YC.at[s.h], yr_sem.at[s.k, 0])
        return finish(s, acc, [W(s, y, t, c), W(s, y, t, 1 - c), far.at[y], YC.at[s.h]], [near.at[y]])

    acc = jnp.zeros((8, 128), F32)
    queue, line = list(FIRST_Y), FIRST_Z + FIRST_Y

    def more(n):
        for s in queue[:n]:
            y_send(s)
        del queue[:n]

    more(2)
    for n in range(len(line) + 2):
        if n < len(line):
            s = line[n]
            if s.two:
                ready(s)
                chain2(s, (0, 1))
                more(2)
            else:
                chain(s, (0, 1))
                more(1)
        if 1 <= n <= len(line):
            s = line[n - 1]
            (chain2 if s.two else chain)(s, (2,))
        if n >= 2:
            s = line[n - 2]
            if s.two:
                y_send2(s)
            else:
                acc = chain_end(s, acc)
    for s in FIRST_Z:
        acc = end2(s, acc)

    for s in SUBS:
        half(s).wait_send()
        for q in range(3):
            z_copy(s, q)[0].wait_send()
        if s.two:
            y_copy2(s).wait_send()
        else:
            for q in range(4):
                y_copy(s, q).wait_send()
    for copy in extra:
        copy.wait()

    NB[0] = acc
    copy = remote(NB.at[0], NB.at[1], ns_sem.at[0], nr_sem.at[0], partner)
    copy.start()
    copy.wait()
    NB[2] = NB[0] + NB[1]
    copy = remote(NB.at[2], NB.at[3], ns_sem.at[1], nr_sem.at[1], across)
    copy.start()
    copy.wait()
    NB[4] = NB[2] + NB[3]
    copies = [remote(NB.at[4], NB.at[4 + d], ns_sem.at[1 + d], nr_sem.at[1 + d], others[d - 1]) for d in range(1, NZ)]
    for copy in copies:
        copy.start()
    for copy in copies:
        copy.wait()
    squares = jnp.sum(NB[4] + NB[5] + NB[6] + NB[7], keepdims=True)
    factor = jnp.minimum(1.0, 0.5 * lax.rsqrt(squares / COUNT + 1e-30))

    def adamw(s):
        m_ref, v_ref, w_ref, out = state(s, MA, MB), state(s, VA, VB), state(s, OA, OB), W(s, y, z, c)

        def one(j, carry):
            ix = tile(s, j)
            g = G(s)[ix].astype(F32) * factor
            m = 0.9 * m_ref[ix] + 0.1 * g
            v = 0.95 * v_ref[ix] + 0.05 * g * g
            w = w_ref[ix].astype(F32)
            m_ref[ix] = m
            v_ref[ix] = v
            out[ix] = (w - 0.02 * (m * lax.rsqrt(v + 1e-8) + 0.1 * w)).astype(BF16)
            return carry

        lax.fori_loop(0, STEPS, one, 0)

    def piece(s, t):
        return W(s, slice(None) if s.two else y, t, c)

    def z_go(s, n, t, direction):
        ref = piece(s, t)
        return remote(ref, ref, zs_sem.at[s.k, n], zr_sem.at[s.k, t], z_dev(direction))

    def y_go(s, n, t):
        ref = W(s, y, t, c)
        return remote(ref, ref, ys_sem.at[s.k, n], yr_sem.at[s.k, t], across)

    def core_go(s, n, yy):
        ref = W(s, yy, slice(None), c)
        return remote(ref, ref, ds_sem.at[s.k, n], dr_sem.at[s.k, n], partner)

    def z_own(s):
        z_go(s, 0, z, away).start()

        @pl.when(inner)
        def _():
            z_go(s, 1, z, toward).start()

    events = [(1 - r, away), (2, toward), (3, toward)]

    def z_events(s):
        for e, (t, direction) in enumerate(events):
            t = absolute(t)
            got(piece(s, t), zr_sem.at[s.k, t])

            @pl.when(inner)
            def _():
                z_go(s, 2 + e, t, direction).start()

            if not s.two:
                y_go(s, 1 + e, t).start()
        if s.two:
            core_go(s, 0, slice(None)).start()
        else:
            core_go(s, 0, y).start()

    def y_end(s):
        for t in range(NZ):
            got(W(s, 1 - y, t, c), yr_sem.at[s.k, t])
        core_go(s, 1, 1 - y).start()

    def own(s):
        adamw(s)
        if s.two:
            y_go(s, 0, z).start()
        else:
            z_own(s)
            y_go(s, 0, z).start()

    def own2(s):
        got(W(s, 1 - y, z, c), yr_sem.at[s.k, z])
        z_own(s)

    own(FIRST_Y[0])
    for s in FIRST_Z:
        own(s)
    own(FIRST_Y[1])
    ended = 0
    for n, s in enumerate(FIRST_Y):
        if n + 2 < len(FIRST_Y):
            own(FIRST_Y[n + 2])
        if n + 2 == len(FIRST_Y):
            own2(FIRST_Z[0])
        if n + 1 == len(FIRST_Y):
            own2(FIRST_Z[1])
        z_events(s)
        if ended + 1 <= (2 * n) // 3 - 1:
            y_end(FIRST_Y[ended])
            ended += 1
    for s in FIRST_Z:
        y_end(FIRST_Y[ended])
        ended += 1
        z_events(s)
    while ended < len(FIRST_Y):
        y_end(FIRST_Y[ended])
        ended += 1

    for s in SUBS:
        if s.two:
            got(W(s, slice(None), slice(None), 1 - c), dr_sem.at[s.k, 0])
            core_go(s, 0, slice(None)).wait_send()
            y_go(s, 0, z).wait_send()
        else:
            got(W(s, y, slice(None), 1 - c), dr_sem.at[s.k, 0])
            got(W(s, 1 - y, slice(None), 1 - c), dr_sem.at[s.k, 1])
            core_go(s, 0, y).wait_send()
            core_go(s, 1, 1 - y).wait_send()
            for n in range(4):
                y_go(s, n, z).wait_send()
        z_go(s, 0, z, away).wait_send()

        @pl.when(inner)
        def _():
            for n in range(1, 5):
                z_go(s, n, z, away).wait_send()


def write_out(WG, WU, WB, MA, MB, VA, VB, *refs):
    outs, sem = refs[:9], refs[9]
    copies = []
    for src, dst in ((WG, outs[0]), (WU, outs[1]), (WB, outs[2])):
        for l in range(L):
            copies += [(src.at[l, yy], dst.at[l, yy]) for yy in range(NY)]
    for A, B, first in ((MA, MB, 3), (VA, VB, 6)):
        copies += [(A.at[0], outs[first]), (A.at[1], outs[first + 1]), (B, outs[first + 2])]
    copies = [pltpu.make_async_copy(src, dst, sem.at[n]) for n, (src, dst) in enumerate(copies)]
    for copy in copies:
        copy.start()
    for copy in copies:
        copy.wait()


def solution(mesh):
    nh = len([s for s in FIRST_Y if s.kind == "B"])
    hbm = pl.BlockSpec(memory_space=pltpu.MemorySpace.HBM)
    vmem = pl.BlockSpec(memory_space=pltpu.MemorySpace.VMEM)
    held = [
        ((L, NY, NZ, NC, RA, FF), BF16),
        ((L, NY, NZ, NC, RA, FF), BF16),
        ((L, NY, NZ, NC, RB, D), BF16),
        ((2, L, RA, FF), F32),
        ((L, RB, D), F32),
        ((2, L, RA, FF), F32),
        ((L, RB, D), F32),
    ]

    def step(*arrays):
        terms, weights, m, v = (arrays[i : i + 3] for i in (0, 3, 6, 9))

        def split(x):
            rows = x.shape[-2] // 16
            return x.reshape(L, NY, NZ, NC, rows, x.shape[-1])

        kept = pl.pallas_call(
            body,
            name="step",
            out_shape=[pltpu.VMEM(shape, dtype) for shape, dtype in held],
            in_specs=[hbm] * 12,
            out_specs=[vmem] * 7,
            scratch_shapes=[
                pltpu.VMEM((8, NZ, RA, CA), BF16),
                pltpu.VMEM((nh, NZ, HB, D), BF16),
                pltpu.VMEM((2, HB, D), BF16),
                pltpu.VMEM((8, 2, 3, RA, CA), BF16),
                pltpu.VMEM((nh, 2, 3, HB, D), BF16),
                pltpu.VMEM((2, 2, 3, NY, HB, D), BF16),
                pltpu.VMEM((8, RA, CA), BF16),
                pltpu.VMEM((4, HB, D), BF16),
                pltpu.VMEM((2, L, RA, FF), BF16),
                pltpu.VMEM((L, RB, D), BF16),
                pltpu.VMEM((8, 8, 128), F32),
                pltpu.SemaphoreType.DMA((NS,)),
                pltpu.SemaphoreType.DMA((9,)),
                pltpu.SemaphoreType.DMA((NS, 2)),
                pltpu.SemaphoreType.DMA((NS, 2)),
                pltpu.SemaphoreType.DMA((NS, 4)),
                pltpu.SemaphoreType.DMA((NS, 4)),
                pltpu.SemaphoreType.DMA((NS, 5)),
                pltpu.SemaphoreType.DMA((NS, 6)),
                pltpu.SemaphoreType.DMA((5,)),
                pltpu.SemaphoreType.DMA((5,)),
            ],
            compiler_params=pltpu.CompilerParams(collective_id=0, has_side_effects=True, vmem_limit_bytes=28 * 2**20),
        )(*(split(t[0]) for t in terms), *(split(w) for w in weights), *m, *v)

        outs = pl.pallas_call(
            write_out,
            name="write_out",
            out_shape=[jax.ShapeDtypeStruct((L, NY, NZ, NC, RA, FF), BF16)] * 2
            + [jax.ShapeDtypeStruct((L, NY, NZ, NC, RB, D), BF16)]
            + ([jax.ShapeDtypeStruct((L, RA, FF), F32)] * 2 + [jax.ShapeDtypeStruct((L, RB, D), F32)]) * 2,
            in_specs=[vmem] * 7,
            out_specs=[hbm] * 9,
            scratch_shapes=[pltpu.SemaphoreType.DMA((18,))],
            compiler_params=pltpu.CompilerParams(vmem_limit_bytes=2 * 2**20),
        )(*kept)
        whole = [x.reshape(L, -1, x.shape[-1]) for x in outs[:3]]
        return (*whole, *outs[3:])

    all_of, cut = P(None, None, None), P(None, "dp", None)
    return jax.shard_map(
        step,
        mesh=mesh,
        in_specs=(P(("rep", "dp"), None, None, None),) * 3 + (all_of,) * 3 + (cut,) * 6,
        out_specs=(P("rep", None, None),) * 3 + (P("rep", "dp", None),) * 6,
        check_vma=False,
    )
```

```python
import jax
import jax.numpy as jnp
from jax import lax
from jax.experimental import pallas as pl
from jax.experimental.pallas import tpu as pltpu
from jax.sharding import PartitionSpec as P

F32, BF16 = jnp.float32, jnp.bfloat16
NY, NZ, NC = 2, 4, 2
L, D, FF = 2, 896, 2560
RA, RB = D // 16, FF // 16
CA, HB = FF // 2, RB // 2
COUNT = 3 * L * D * FF


class Sub:
    def __init__(self, k, kind, m, l, h, i, two):
        self.k, self.kind, self.m, self.l, self.h, self.i, self.two = k, kind, m, l, h, i, two

    @property
    def cols(self):
        return pl.ds(self.h * CA, CA)

    @property
    def rows(self):
        return pl.ds(self.h * HB, HB)


def subunits():
    subs = []
    for m in range(2):
        for l in range(L):
            for h in range(2):
                subs.append(Sub(len(subs), "A", m, l, h, len(subs), False))
    for l in range(L):
        for h in range(2):
            subs.append(Sub(len(subs), "B", 0, l, h, l * 2 + h, l == 1))
    return subs


SUBS = subunits()
FIRST_Y = [s for s in SUBS if not s.two]
FIRST_Z = [s for s in SUBS if s.two]
NS = len(SUBS)
STEPS = 5


def tile(sub, j):
    if sub.kind == "A":
        return (slice(None), pl.ds(pl.multiple_of(j * 256, 256), 256))
    return (pl.ds(pl.multiple_of(j * 16, 16), 16), slice(None))


def body(
    g_gate, g_up, g_down, w_gate, w_up, w_down, mg, mu, md, vg, vu, vd,
    WG0, WG1, WU0, WU1, WB0, WB1, MA, MB, VA, VB,
    YA, YB, YC, ZA, ZB, ZC, GA, GB, OA, OB, NB,
    ld_sem, mv_sem, ds_sem, dr_sem, ys_sem, yr_sem, zs_sem, zr_sem, ns_sem, nr_sem,
):
    me = lax.axis_index("dp")
    c = me % 2
    z = (me // 2) % NZ
    y = me // (2 * NZ)
    side = z // 2
    r = jnp.where(side == 0, z, 3 - z)
    inner = r == 1
    away, toward = side, 1 - side

    def dev(yy, zz, cc):
        return {"dp": (yy * NZ + zz) * NC + cc}

    partner = dev(y, z, 1 - c)
    across = dev(1 - y, z, c)
    away_dev = dev(y, z + 1 - 2 * away, c)

    def z_dev(direction):
        return dev(y, z + 1 - 2 * direction, c)

    def absolute(t):
        return t + side * (3 - 2 * t)

    def slot(t, direction):
        return jnp.clip(t - 1 + direction, 0, 2)

    def W(s, yy, zz, cc):
        if s.kind == "A":
            return ((WG0, WG1), (WU0, WU1))[s.m][s.l].at[yy, zz, cc, :, s.cols]
        return (WB0, WB1)[s.l].at[yy, zz, cc, s.rows, :]

    def G_in(s, cc):
        if s.kind == "A":
            return (g_gate, g_up)[s.m].at[s.l, :, :, cc, :, s.cols]
        return g_down.at[s.l, :, :, cc, s.rows, :]

    def Y(s, t):
        return YA.at[s.i, t] if s.kind == "A" else YB.at[s.i, t]

    def Z(s, direction, sl):
        return ZA.at[s.i, direction, sl] if s.kind == "A" else ZB.at[s.i, direction, sl]

    def Z2(s, direction, sl):
        return ZC.at[s.h, direction, sl]

    def G(s):
        return GA.at[s.i] if s.kind == "A" else GB.at[s.i]

    def state(s, A, B):
        return A.at[s.m, s.l, :, s.cols] if s.kind == "A" else B.at[s.l, s.rows, :]

    def remote(src, dst, ss, rs, device):
        return pltpu.make_async_remote_copy(src, dst, ss, rs, device_id=device, device_id_type=pl.DeviceIdType.MESH)

    def got(ref, sem):
        remote(ref, ref, sem, sem, partner).wait_recv()

    def sent(ref, sem):
        remote(ref, ref, sem, sem, partner).wait_send()

    barrier = pltpu.get_barrier_semaphore()

    def greet(peer):
        pl.semaphore_signal(barrier, inc=1, device_id=peer, device_id_type=pl.DeviceIdType.MESH)

    greet(across)
    greet(z_dev(away))

    @pl.when(inner)
    def _():
        greet(z_dev(toward))

    greet(partner)
    pl.semaphore_wait(barrier, 3 + jnp.where(inner, 1, 0))

    def load(s):
        return pltpu.make_async_copy(G_in(s, c), W(s, slice(None), slice(None), c), ld_sem.at[s.k])

    y_order = [3, 2, 1 - r, r]

    def halves(s):
        if s is not FIRST_Y[0]:
            return [remote(G_in(s, 1 - c), W(s, slice(None), slice(None), c), ds_sem.at[s.k, 0], dr_sem.at[s.k, 0], partner)]
        out = []
        for q in range(4):
            t = absolute(y_order[q])
            out.append(remote(G_in(s, 1 - c).at[1 - y, t], W(s, 1 - y, t, c), ds_sem.at[s.k, q], dr_sem.at[s.k, q], partner))
        out.append(remote(G_in(s, 1 - c).at[y], W(s, y, slice(None), c), ds_sem.at[s.k, 4], dr_sem.at[s.k, 4], partner))
        return out

    start_order = [FIRST_Y[0], FIRST_Z[0], FIRST_Y[1], FIRST_Z[1], *FIRST_Y[2:]]
    for s in start_order:
        load(s).start()
        for copy in halves(s):
            copy.start()
    chip = (y, z)
    extra = []
    for n, (src, A) in enumerate(((w_gate, OA), (w_up, OA))):
        extra.append(pltpu.make_async_copy(src.at[:, y, z, c], A.at[n], mv_sem.at[n]))
    extra.append(pltpu.make_async_copy(w_down.at[:, y, z, c], OB, mv_sem.at[2]))
    for n, (src, dst) in enumerate(((mg, MA.at[0]), (mu, MA.at[1]), (md, MB), (vg, VA.at[0]), (vu, VA.at[1]), (vd, VB))):
        extra.append(pltpu.make_async_copy(src, dst, mv_sem.at[3 + n]))
    for copy in extra:
        copy.start()

    def ready(s):
        load(s).wait()
        got(W(s, slice(None), slice(None), 1 - c), dr_sem.at[s.k, 0])

    def total(s, srcs, maybe):
        def at(ix):
            out = None
            for ref in srcs:
                one = ref[ix].astype(F32)
                out = one if out is None else out + one
            for ref in maybe:
                out = out + jnp.where(inner, ref[ix].astype(F32), 0.0)
            return out

        return at

    def add_into(s, dst, srcs, maybe=()):
        value = total(s, srcs, maybe)

        def one(j, carry):
            ix = tile(s, j)
            dst[ix] = value(ix).astype(BF16)
            return carry

        lax.fori_loop(0, STEPS, one, 0)

    def finish(s, acc, srcs, maybe=()):
        value = total(s, srcs, maybe)

        def one(j, carry):
            ix = tile(s, j)
            g = value(ix).astype(BF16)
            G(s)[ix] = g
            g = g.astype(F32)
            g = g * g
            for a in range(g.shape[0] // 8):
                for b in range(g.shape[1] // 128):
                    carry = carry + g[a * 8 : a * 8 + 8, b * 128 : b * 128 + 128]
            return carry

        return lax.fori_loop(0, STEPS, one, acc)

    steps = [(3, away), (2, away), (1 - r, jnp.where(inner, toward, away))]
    def y_copy(s, q):
        t = absolute(y_order[q])
        return remote(W(s, 1 - y, t, 1 - c), Y(s, t), ys_sem.at[s.k, q], yr_sem.at[s.k, q], across)

    def y_send(s):
        whole = s is not FIRST_Y[0]
        if whole:
            ready(s)
        else:
            load(s).wait()
        for q in range(4):
            t = absolute(y_order[q])
            if not whole:
                got(W(s, 1 - y, t, 1 - c), dr_sem.at[s.k, q])
            dst = W(s, 1 - y, t, 1 - c)
            add_into(s, dst, [W(s, 1 - y, t, c), dst])
            y_copy(s, q).start()
        if not whole:
            got(W(s, y, slice(None), 1 - c), dr_sem.at[s.k, 4])

    def z_copy(s, q):
        t, direction = absolute(steps[q][0]), steps[q][1]
        sl = slot(t, direction)
        ref = Z(s, direction, sl) if not s.two else Z2(s, direction, sl)
        return remote(ref, ref, zs_sem.at[s.k, q], zr_sem.at[s.k, direction * 3 + sl], z_dev(direction)), ref, sl, t, direction

    def chain(s, qs):
        for q in qs:
            copy, ref, sl, t, direction = z_copy(s, q)
            got(Y(s, t), yr_sem.at[s.k, q])

            @pl.when(inner)
            def _():
                got(ref, zr_sem.at[s.k, direction * 3 + sl])

            add_into(s, ref, [W(s, y, t, c), W(s, y, t, 1 - c), Y(s, t)], [ref])
            copy.start()

    def chain_end(s, acc):
        t = absolute(r)
        got(Y(s, t), yr_sem.at[s.k, 3])
        view = Z if not s.two else Z2
        near, far = slot(t, away), slot(t, toward)
        got(view(s, toward, far), zr_sem.at[s.k, toward * 3 + far])

        @pl.when(inner)
        def _():
            got(view(s, away, near), zr_sem.at[s.k, away * 3 + near])

        return finish(s, acc, [W(s, y, t, c), W(s, y, t, 1 - c), Y(s, t), view(s, toward, far)], [view(s, away, near)])

    def chain2(s, qs):
        for q in qs:
            copy, ref, sl, t, direction = z_copy(s, q)

            @pl.when(inner)
            def _():
                got(ref, zr_sem.at[s.k, direction * 3 + sl])

            for yy in range(2):
                add_into(s, ref.at[yy], [W(s, yy, t, c), W(s, yy, t, 1 - c)], [ref.at[yy]])
            copy.start()

    def ends2(s):
        t = absolute(r)
        return t, Z2(s, toward, slot(t, toward)), Z2(s, away, slot(t, away))

    def y_copy2(s):
        t, far, near = ends2(s)
        return remote(far.at[1 - y], YC.at[s.h], ys_sem.at[s.k, 0], yr_sem.at[s.k, 0], across)

    def y_send2(s):
        t, far, near = ends2(s)
        got(far, zr_sem.at[s.k, toward * 3 + slot(t, toward)])

        @pl.when(inner)
        def _():
            got(near, zr_sem.at[s.k, away * 3 + slot(t, away)])

        dst = far.at[1 - y]
        add_into(s, dst, [W(s, 1 - y, t, c), W(s, 1 - y, t, 1 - c), dst], [near.at[1 - y]])
        y_copy2(s).start()

    def end2(s, acc):
        t, far, near = ends2(s)
        got(YC.at[s.h], yr_sem.at[s.k, 0])
        return finish(s, acc, [W(s, y, t, c), W(s, y, t, 1 - c), far.at[y], YC.at[s.h]], [near.at[y]])

    acc = jnp.zeros((8, 128), F32)
    queue, line = list(FIRST_Y), FIRST_Z + FIRST_Y

    def more(n):
        for s in queue[:n]:
            y_send(s)
        del queue[:n]

    more(1)
    for n in range(len(line) + 2):
        if n < len(line):
            s = line[n]
            if s.two:
                ready(s)
                chain2(s, (0, 1))
                more(2)
            else:
                chain(s, (0, 1))
                more(1 if n > 2 else 2)
        if 1 <= n <= len(line):
            s = line[n - 1]
            (chain2 if s.two else chain)(s, (2,))
        if n >= 2:
            s = line[n - 2]
            if not s.two:
                acc = chain_end(s, acc)
        if n in (6, 7):
            y_send2(FIRST_Z[n - 6])
    for s in FIRST_Z:
        acc = end2(s, acc)

    for s in SUBS:
        for copy in halves(s):
            copy.wait_send()
        for q in range(3):
            z_copy(s, q)[0].wait_send()
        if s.two:
            y_copy2(s).wait_send()
        else:
            for q in range(4):
                y_copy(s, q).wait_send()
    for copy in extra:
        copy.wait()

    NB[me] = acc
    copies = []
    for d in range(1, 16):
        peer = (me + d) % 16
        copies.append((remote(NB.at[me], NB.at[me], ns_sem.at[d - 1], nr_sem.at[me], {"dp": peer}), peer))
    for copy, _ in copies:
        copy.start()
    for _, peer in copies:
        got(NB.at[peer], nr_sem.at[peer])
    for copy, _ in copies:
        copy.wait_send()
    squares = NB[0]
    for d in range(1, 16):
        squares = squares + NB[d]
    squares = jnp.sum(squares, keepdims=True)
    factor = jnp.minimum(1.0, 0.5 * lax.rsqrt(squares / COUNT + 1e-30))

    def adamw(s):
        m_ref, v_ref, w_ref, out = state(s, MA, MB), state(s, VA, VB), state(s, OA, OB), W(s, y, z, c)

        def one(j, carry):
            ix = tile(s, j)
            g = G(s)[ix].astype(F32) * factor
            m = 0.9 * m_ref[ix] + 0.1 * g
            v = 0.95 * v_ref[ix] + 0.05 * g * g
            w = w_ref[ix].astype(F32)
            m_ref[ix] = m
            v_ref[ix] = v
            out[ix] = (w - 0.02 * (m * lax.rsqrt(v + 1e-8) + 0.1 * w)).astype(BF16)
            return carry

        lax.fori_loop(0, STEPS, one, 0)

    def piece(s, t):
        return W(s, slice(None) if s.two else y, t, c)

    def z_go(s, n, t, direction):
        ref = piece(s, t)
        return remote(ref, ref, zs_sem.at[s.k, n], zr_sem.at[s.k, t], z_dev(direction))

    def y_go(s, n, t):
        ref = W(s, y, t, c)
        return remote(ref, ref, ys_sem.at[s.k, n], yr_sem.at[s.k, t], across)

    def core_go(s, n, yy):
        ref = W(s, yy, slice(None), c)
        return remote(ref, ref, ds_sem.at[s.k, n], dr_sem.at[s.k, n], partner)

    def z_own(s):
        z_go(s, 0, z, away).start()

        @pl.when(inner)
        def _():
            z_go(s, 1, z, toward).start()

    events = [(1 - r, away), (2, toward), (3, toward)]

    def z_events(s):
        for e, (t, direction) in enumerate(events):
            t = absolute(t)
            got(piece(s, t), zr_sem.at[s.k, t])

            @pl.when(inner)
            def _():
                z_go(s, 2 + e, t, direction).start()

            if not s.two:
                y_go(s, 1 + e, t).start()
        if s.two:
            core_go(s, 0, slice(None)).start()
        else:
            core_go(s, 0, y).start()

    def y_end(s):
        for t in range(NZ):
            got(W(s, 1 - y, t, c), yr_sem.at[s.k, t])
        core_go(s, 1, 1 - y).start()

    def own(s):
        adamw(s)
        if s.two:
            y_go(s, 0, z).start()
        else:
            z_own(s)
            y_go(s, 0, z).start()

    def own2(s):
        got(W(s, 1 - y, z, c), yr_sem.at[s.k, z])
        z_own(s)

    own(FIRST_Y[0])
    for s in FIRST_Z:
        own(s)
    own(FIRST_Y[1])
    ended = 0
    for n, s in enumerate(FIRST_Y):
        if n + 2 < len(FIRST_Y):
            own(FIRST_Y[n + 2])
        if n + 2 == len(FIRST_Y):
            own2(FIRST_Z[0])
        if n + 1 == len(FIRST_Y):
            own2(FIRST_Z[1])
        z_events(s)
        if ended + 1 <= (2 * n) // 3 - 1:
            y_end(FIRST_Y[ended])
            ended += 1
    for s in FIRST_Z:
        y_end(FIRST_Y[ended])
        ended += 1
        z_events(s)
    while ended < len(FIRST_Y):
        y_end(FIRST_Y[ended])
        ended += 1

    for s in SUBS:
        if s.two:
            got(W(s, slice(None), slice(None), 1 - c), dr_sem.at[s.k, 0])
            core_go(s, 0, slice(None)).wait_send()
            y_go(s, 0, z).wait_send()
        else:
            got(W(s, y, slice(None), 1 - c), dr_sem.at[s.k, 0])
            got(W(s, 1 - y, slice(None), 1 - c), dr_sem.at[s.k, 1])
            core_go(s, 0, y).wait_send()
            core_go(s, 1, 1 - y).wait_send()
            for n in range(4):
                y_go(s, n, z).wait_send()
        z_go(s, 0, z, away).wait_send()

        @pl.when(inner)
        def _():
            for n in range(1, 5):
                z_go(s, n, z, away).wait_send()


def flush(copies, sem):
    copies = [pltpu.make_async_copy(src, dst, sem.at[n]) for n, (src, dst) in enumerate(copies)]
    for copy in copies:
        copy.start()
    for copy in copies:
        copy.wait()


def write_w(WG0, WG1, WU0, WU1, WB0, WB1, gate, up, down, sem):
    pairs = ((WG0, WG1), gate), ((WU0, WU1), up), ((WB0, WB1), down)
    flush([(pair[l].at[yy], dst.at[l, yy]) for pair, dst in pairs for l in range(L) for yy in range(NY)], sem)


def write_state(MA, MB, VA, VB, *refs):
    pairs = zip((MA.at[0], MA.at[1], MB, VA.at[0], VA.at[1], VB), refs[:6], strict=True)
    flush(list(pairs), refs[6])


def solution(mesh):
    nh = len([s for s in FIRST_Y if s.kind == "B"])
    hbm = pl.BlockSpec(memory_space=pltpu.MemorySpace.HBM)
    vmem = pl.BlockSpec(memory_space=pltpu.MemorySpace.VMEM)
    held = [
        *[((NY, NZ, NC, RA, FF), BF16)] * 4,
        *[((NY, NZ, NC, RB, D), BF16)] * 2,
        ((2, L, RA, FF), F32),
        ((L, RB, D), F32),
        ((2, L, RA, FF), F32),
        ((L, RB, D), F32),
    ]

    def step(*arrays):
        terms, weights, m, v = (arrays[i : i + 3] for i in (0, 3, 6, 9))

        def split(x):
            rows = x.shape[-2] // 16
            return x.reshape(L, NY, NZ, NC, rows, x.shape[-1])

        kept = pl.pallas_call(
            body,
            name="step",
            out_shape=[pltpu.VMEM(shape, dtype) for shape, dtype in held],
            in_specs=[hbm] * 12,
            out_specs=[vmem] * 10,
            scratch_shapes=[
                pltpu.VMEM((8, NZ, RA, CA), BF16),
                pltpu.VMEM((nh, NZ, HB, D), BF16),
                pltpu.VMEM((2, HB, D), BF16),
                pltpu.VMEM((8, 2, 3, RA, CA), BF16),
                pltpu.VMEM((nh, 2, 3, HB, D), BF16),
                pltpu.VMEM((2, 2, 3, NY, HB, D), BF16),
                pltpu.VMEM((8, RA, CA), BF16),
                pltpu.VMEM((4, HB, D), BF16),
                pltpu.VMEM((2, L, RA, FF), BF16),
                pltpu.VMEM((L, RB, D), BF16),
                pltpu.VMEM((16, 8, 128), F32),
                pltpu.SemaphoreType.DMA((NS,)),
                pltpu.SemaphoreType.DMA((9,)),
                pltpu.SemaphoreType.DMA((NS, 5)),
                pltpu.SemaphoreType.DMA((NS, 5)),
                pltpu.SemaphoreType.DMA((NS, 4)),
                pltpu.SemaphoreType.DMA((NS, 4)),
                pltpu.SemaphoreType.DMA((NS, 5)),
                pltpu.SemaphoreType.DMA((NS, 6)),
                pltpu.SemaphoreType.DMA((15,)),
                pltpu.SemaphoreType.DMA((16,)),
            ],
            compiler_params=pltpu.CompilerParams(collective_id=0, has_side_effects=True, vmem_limit_bytes=24 * 2**20),
        )(*(split(t[0]) for t in terms), *(split(w) for w in weights), *m, *v)

        whole = pl.pallas_call(
            write_w,
            name="write_w",
            out_shape=[jax.ShapeDtypeStruct((L, NY, NZ, NC, RA, FF), BF16)] * 2
            + [jax.ShapeDtypeStruct((L, NY, NZ, NC, RB, D), BF16)],
            in_specs=[vmem] * 6,
            out_specs=[hbm] * 3,
            scratch_shapes=[pltpu.SemaphoreType.DMA((12,))],
            compiler_params=pltpu.CompilerParams(vmem_limit_bytes=24 * 2**20),
        )(*kept[:6])
        state = pl.pallas_call(
            write_state,
            name="write_state",
            out_shape=([jax.ShapeDtypeStruct((L, RA, FF), F32)] * 2 + [jax.ShapeDtypeStruct((L, RB, D), F32)]) * 2,
            in_specs=[vmem] * 4,
            out_specs=[hbm] * 6,
            scratch_shapes=[pltpu.SemaphoreType.DMA((6,))],
            compiler_params=pltpu.CompilerParams(vmem_limit_bytes=24 * 2**20),
        )(*kept[6:])
        outs = [*whole, *state]
        whole = [x.reshape(L, -1, x.shape[-1]) for x in outs[:3]]
        return (*whole, *outs[3:])

    all_of, cut = P(None, None, None), P(None, "dp", None)
    return jax.shard_map(
        step,
        mesh=mesh,
        in_specs=(P(("rep", "dp"), None, None, None),) * 3 + (all_of,) * 3 + (cut,) * 6,
        out_specs=(P("rep", None, None),) * 3 + (P("rep", "dp", None),) * 6,
        check_vma=False,
    )
```

```python
import jax
import jax.numpy as jnp
from jax import lax
from jax.experimental import pallas as pl
from jax.experimental.pallas import tpu as pltpu
from jax.sharding import PartitionSpec as P

F32, BF16 = jnp.float32, jnp.bfloat16
NY, NZ, NC = 2, 4, 2
L, D, FF = 2, 896, 2560
RA, RB = D // 16, FF // 16
CA, HB = FF // 2, RB // 2
COUNT = 3 * L * D * FF


class Sub:
    def __init__(self, k, kind, m, l, h, i, two):
        self.k, self.kind, self.m, self.l, self.h, self.i, self.two = k, kind, m, l, h, i, two

    @property
    def cols(self):
        return pl.ds(self.h * CA, CA)

    @property
    def rows(self):
        return pl.ds(self.h * HB, HB)


def subunits():
    subs = []
    for m in range(2):
        for l in range(L):
            for h in range(2):
                subs.append(Sub(len(subs), "A", m, l, h, len(subs), False))
    for l in range(L):
        for h in range(2):
            subs.append(Sub(len(subs), "B", 0, l, h, l * 2 + h, l == 1))
    return subs


SUBS = subunits()
FIRST_Y = [s for s in SUBS if not s.two]
FIRST_Z = [s for s in SUBS if s.two]
NS = len(SUBS)
STEPS = 5


def tile(sub, j):
    if sub.kind == "A":
        return (slice(None), pl.ds(pl.multiple_of(j * 256, 256), 256))
    return (pl.ds(pl.multiple_of(j * 16, 16), 16), slice(None))


def body(
    g_gate, g_up, g_down, w_gate, w_up, w_down, mg, mu, md, vg, vu, vd,
    WG0, WG1, WU0, WU1, WB0, WB1, MA, MB, VA, VB,
    YA, YB, YC, ZA, ZB, ZC, GA, GB, OA, OB, NB,
    ld_sem, mv_sem, ds_sem, dr_sem, ys_sem, yr_sem, zs_sem, zr_sem, ns_sem, nr_sem,
):
    me = lax.axis_index("dp")
    c = me % 2
    z = (me // 2) % NZ
    y = me // (2 * NZ)
    side = z // 2
    r = jnp.where(side == 0, z, 3 - z)
    inner = r == 1
    away, toward = side, 1 - side

    def dev(yy, zz, cc):
        return {"dp": (yy * NZ + zz) * NC + cc}

    partner = dev(y, z, 1 - c)
    across = dev(1 - y, z, c)
    away_dev = dev(y, z + 1 - 2 * away, c)

    def z_dev(direction):
        return dev(y, z + 1 - 2 * direction, c)

    def absolute(t):
        return t + side * (3 - 2 * t)

    def slot(t, direction):
        return jnp.clip(t - 1 + direction, 0, 2)

    def W(s, yy, zz, cc):
        if s.kind == "A":
            return ((WG0, WG1), (WU0, WU1))[s.m][s.l].at[yy, zz, cc, :, s.cols]
        return (WB0, WB1)[s.l].at[yy, zz, cc, s.rows, :]

    def G_in(s, cc):
        if s.kind == "A":
            return (g_gate, g_up)[s.m].at[s.l, :, :, cc, :, s.cols]
        return g_down.at[s.l, :, :, cc, s.rows, :]

    def Y(s, t):
        return YA.at[s.i, t] if s.kind == "A" else YB.at[s.i, t]

    def Z(s, direction, sl):
        return ZA.at[s.i, direction, sl] if s.kind == "A" else ZB.at[s.i, direction, sl]

    def Z2(s, direction, sl):
        return ZC.at[s.h, direction, sl]

    def G(s):
        return GA.at[s.i] if s.kind == "A" else GB.at[s.i]

    def state(s, A, B):
        return A.at[s.m, s.l, :, s.cols] if s.kind == "A" else B.at[s.l, s.rows, :]

    def remote(src, dst, ss, rs, device):
        return pltpu.make_async_remote_copy(src, dst, ss, rs, device_id=device, device_id_type=pl.DeviceIdType.MESH)

    def got(ref, sem):
        remote(ref, ref, sem, sem, partner).wait_recv()

    def sent(ref, sem):
        remote(ref, ref, sem, sem, partner).wait_send()

    barrier = pltpu.get_barrier_semaphore()

    def greet(peer):
        pl.semaphore_signal(barrier, inc=1, device_id=peer, device_id_type=pl.DeviceIdType.MESH)

    greet(across)
    greet(z_dev(away))

    @pl.when(inner)
    def _():
        greet(z_dev(toward))

    greet(partner)
    pl.semaphore_wait(barrier, 3 + jnp.where(inner, 1, 0))

    def load(s):
        return pltpu.make_async_copy(G_in(s, c), W(s, slice(None), slice(None), c), ld_sem.at[s.k])

    y_order = [3, 2, 1 - r, r]

    def halves(s):
        if s is not FIRST_Y[0]:
            return [remote(G_in(s, 1 - c), W(s, slice(None), slice(None), c), ds_sem.at[s.k, 0], dr_sem.at[s.k, 0], partner)]
        out = []
        for q in range(4):
            t = absolute(y_order[q])
            out.append(remote(G_in(s, 1 - c).at[1 - y, t], W(s, 1 - y, t, c), ds_sem.at[s.k, q], dr_sem.at[s.k, q], partner))
        out.append(remote(G_in(s, 1 - c).at[y], W(s, y, slice(None), c), ds_sem.at[s.k, 4], dr_sem.at[s.k, 4], partner))
        return out

    start_order = [FIRST_Y[0], FIRST_Z[0], FIRST_Y[1], FIRST_Z[1], *FIRST_Y[2:]]
    for s in start_order:
        load(s).start()
        for copy in halves(s):
            copy.start()
    chip = (y, z)
    extra = []
    for n, (src, A) in enumerate(((w_gate, OA), (w_up, OA))):
        extra.append(pltpu.make_async_copy(src.at[:, y, z, c], A.at[n], mv_sem.at[n]))
    extra.append(pltpu.make_async_copy(w_down.at[:, y, z, c], OB, mv_sem.at[2]))
    for n, (src, dst) in enumerate(((mg, MA.at[0]), (mu, MA.at[1]), (md, MB), (vg, VA.at[0]), (vu, VA.at[1]), (vd, VB))):
        extra.append(pltpu.make_async_copy(src, dst, mv_sem.at[3 + n]))
    for copy in extra:
        copy.start()

    def ready(s):
        load(s).wait()
        got(W(s, slice(None), slice(None), 1 - c), dr_sem.at[s.k, 0])

    def total(s, srcs, maybe):
        def at(ix):
            out = None
            for ref in srcs:
                one = ref[ix].astype(F32)
                out = one if out is None else out + one
            for ref in maybe:
                out = out + jnp.where(inner, ref[ix].astype(F32), 0.0)
            return out

        return at

    def add_into(s, dst, srcs, maybe=()):
        value = total(s, srcs, maybe)

        def one(j, carry):
            ix = tile(s, j)
            dst[ix] = value(ix).astype(BF16)
            return carry

        lax.fori_loop(0, STEPS, one, 0)

    def finish(s, acc, srcs, maybe=()):
        value = total(s, srcs, maybe)

        def one(j, carry):
            ix = tile(s, j)
            g = value(ix).astype(BF16)
            G(s)[ix] = g
            g = g.astype(F32)
            g = g * g
            for a in range(g.shape[0] // 8):
                for b in range(g.shape[1] // 128):
                    carry = carry + g[a * 8 : a * 8 + 8, b * 128 : b * 128 + 128]
            return carry

        return lax.fori_loop(0, STEPS, one, acc)

    steps = [(3, away), (2, away), (1 - r, jnp.where(inner, toward, away))]
    def y_copy(s, q):
        t = absolute(y_order[q])
        return remote(W(s, 1 - y, t, 1 - c), Y(s, t), ys_sem.at[s.k, q], yr_sem.at[s.k, q], across)

    def y_send(s):
        whole = s is not FIRST_Y[0]
        if whole:
            ready(s)
        else:
            load(s).wait()
        for q in range(4):
            t = absolute(y_order[q])
            if not whole:
                got(W(s, 1 - y, t, 1 - c), dr_sem.at[s.k, q])
            dst = W(s, 1 - y, t, 1 - c)
            add_into(s, dst, [W(s, 1 - y, t, c), dst])
            y_copy(s, q).start()
        if not whole:
            got(W(s, y, slice(None), 1 - c), dr_sem.at[s.k, 4])

    def z_copy(s, q):
        t, direction = absolute(steps[q][0]), steps[q][1]
        sl = slot(t, direction)
        ref = Z(s, direction, sl) if not s.two else Z2(s, direction, sl)
        return remote(ref, ref, zs_sem.at[s.k, q], zr_sem.at[s.k, direction * 3 + sl], z_dev(direction)), ref, sl, t, direction

    def chain(s, qs):
        for q in qs:
            copy, ref, sl, t, direction = z_copy(s, q)
            got(Y(s, t), yr_sem.at[s.k, q])

            @pl.when(inner)
            def _():
                got(ref, zr_sem.at[s.k, direction * 3 + sl])

            add_into(s, ref, [W(s, y, t, c), W(s, y, t, 1 - c), Y(s, t)], [ref])
            copy.start()

    def chain_end(s, acc):
        t = absolute(r)
        got(Y(s, t), yr_sem.at[s.k, 3])
        view = Z if not s.two else Z2
        near, far = slot(t, away), slot(t, toward)
        got(view(s, toward, far), zr_sem.at[s.k, toward * 3 + far])

        @pl.when(inner)
        def _():
            got(view(s, away, near), zr_sem.at[s.k, away * 3 + near])

        return finish(s, acc, [W(s, y, t, c), W(s, y, t, 1 - c), Y(s, t), view(s, toward, far)], [view(s, away, near)])

    def chain2(s, qs):
        for q in qs:
            copy, ref, sl, t, direction = z_copy(s, q)

            @pl.when(inner)
            def _():
                got(ref, zr_sem.at[s.k, direction * 3 + sl])

            for yy in range(2):
                add_into(s, ref.at[yy], [W(s, yy, t, c), W(s, yy, t, 1 - c)], [ref.at[yy]])
            copy.start()

    def ends2(s):
        t = absolute(r)
        return t, Z2(s, toward, slot(t, toward)), Z2(s, away, slot(t, away))

    def y_copy2(s):
        t, far, near = ends2(s)
        return remote(far.at[1 - y], YC.at[s.h], ys_sem.at[s.k, 0], yr_sem.at[s.k, 0], across)

    def y_send2(s):
        t, far, near = ends2(s)
        got(far, zr_sem.at[s.k, toward * 3 + slot(t, toward)])

        @pl.when(inner)
        def _():
            got(near, zr_sem.at[s.k, away * 3 + slot(t, away)])

        dst = far.at[1 - y]
        add_into(s, dst, [W(s, 1 - y, t, c), W(s, 1 - y, t, 1 - c), dst], [near.at[1 - y]])
        y_copy2(s).start()

    def end2(s, acc):
        t, far, near = ends2(s)
        got(YC.at[s.h], yr_sem.at[s.k, 0])
        return finish(s, acc, [W(s, y, t, c), W(s, y, t, 1 - c), far.at[y], YC.at[s.h]], [near.at[y]])

    acc = jnp.zeros((8, 128), F32)
    queue, line = list(FIRST_Y), FIRST_Z + FIRST_Y

    def more(n):
        for s in queue[:n]:
            y_send(s)
        del queue[:n]

    more(1)
    for n in range(len(line) + 2):
        if n < len(line):
            s = line[n]
            if s.two:
                ready(s)
                chain2(s, (0, 1))
                more(2)
            else:
                chain(s, (0, 1))
                more(1 if n > 2 else 2)
        if 1 <= n <= len(line):
            s = line[n - 1]
            (chain2 if s.two else chain)(s, (2,))
        if n >= 2:
            s = line[n - 2]
            if not s.two:
                acc = chain_end(s, acc)
        if n in (6, 7):
            y_send2(FIRST_Z[n - 6])
    for s in FIRST_Z:
        acc = end2(s, acc)

    for s in SUBS:
        for copy in halves(s):
            copy.wait_send()
        for q in range(3):
            z_copy(s, q)[0].wait_send()
        if s.two:
            y_copy2(s).wait_send()
        else:
            for q in range(4):
                y_copy(s, q).wait_send()
    for copy in extra:
        copy.wait()

    NB[me] = acc
    copies = []
    for d in range(1, 16):
        peer = (me + d) % 16
        copies.append((remote(NB.at[me], NB.at[me], ns_sem.at[d - 1], nr_sem.at[me], {"dp": peer}), peer))
    for copy, _ in copies:
        copy.start()
    for _, peer in copies:
        got(NB.at[peer], nr_sem.at[peer])
    for copy, _ in copies:
        copy.wait_send()
    squares = NB[0]
    for d in range(1, 16):
        squares = squares + NB[d]
    squares = jnp.sum(squares, keepdims=True)
    factor = jnp.minimum(1.0, 0.5 * lax.rsqrt(squares / COUNT + 1e-30))

    def adamw(s):
        m_ref, v_ref, w_ref, out = state(s, MA, MB), state(s, VA, VB), state(s, OA, OB), W(s, y, z, c)

        def one(j, carry):
            ix = tile(s, j)
            g = G(s)[ix].astype(F32) * factor
            m = 0.9 * m_ref[ix] + 0.1 * g
            v = 0.95 * v_ref[ix] + 0.05 * g * g
            w = w_ref[ix].astype(F32)
            m_ref[ix] = m
            v_ref[ix] = v
            out[ix] = (w - 0.02 * (m * lax.rsqrt(v + 1e-8) + 0.1 * w)).astype(BF16)
            return carry

        lax.fori_loop(0, STEPS, one, 0)

    def piece(s, t):
        return W(s, slice(None) if s.two else y, t, c)

    def z_go(s, n, t, direction):
        ref = piece(s, t)
        return remote(ref, ref, zs_sem.at[s.k, n], zr_sem.at[s.k, t], z_dev(direction))

    def y_go(s, n, t):
        ref = W(s, y, t, c)
        return remote(ref, ref, ys_sem.at[s.k, n], yr_sem.at[s.k, t], across)

    def core_go(s, n, yy):
        ref = W(s, yy, slice(None), c)
        return remote(ref, ref, ds_sem.at[s.k, n], dr_sem.at[s.k, n], partner)

    def z_own(s):
        z_go(s, 0, z, away).start()

        @pl.when(inner)
        def _():
            z_go(s, 1, z, toward).start()

    events = [(1 - r, away), (2, toward), (3, toward)]

    def pair_go(s, q):
        ref = W(s, slice(None), absolute(y_order[3 - q]), c)
        return remote(ref, ref, ds_sem.at[s.k, q], dr_sem.at[s.k, q], partner)

    def z_events(s):
        for e, (t, direction) in enumerate(events):
            t = absolute(t)
            got(piece(s, t), zr_sem.at[s.k, t])

            @pl.when(inner)
            def _():
                z_go(s, 2 + e, t, direction).start()

            if not s.two:
                y_go(s, 1 + e, t).start()
            else:
                pair_go(s, 1 + e).start()
        if not s.two:
            core_go(s, 0, y).start()

    def last_go(s, q):
        ref = W(s, 1 - y, absolute(y_order[3 - q]), c)
        return remote(ref, ref, ds_sem.at[s.k, 1 + q], dr_sem.at[s.k, 1 + q], partner)

    def y_end(s):
        if s is FIRST_Y[-1]:
            for q, t in enumerate((r, 1 - r, 2, 3)):
                t = absolute(t)
                got(W(s, 1 - y, t, c), yr_sem.at[s.k, t])
                last_go(s, q).start()
            return
        for t in range(NZ):
            got(W(s, 1 - y, t, c), yr_sem.at[s.k, t])
        core_go(s, 1, 1 - y).start()

    def own(s):
        adamw(s)
        if s.two:
            y_go(s, 0, z).start()
        else:
            z_own(s)
            y_go(s, 0, z).start()

    def own2(s):
        got(W(s, 1 - y, z, c), yr_sem.at[s.k, z])
        z_own(s)
        pair_go(s, 0).start()

    own(FIRST_Y[0])
    for s in FIRST_Z:
        own(s)
    own(FIRST_Y[1])
    ended = 0
    for n, s in enumerate(FIRST_Y):
        if n + 2 < len(FIRST_Y):
            own(FIRST_Y[n + 2])
        if n + 2 == len(FIRST_Y):
            own2(FIRST_Z[0])
        if n + 1 == len(FIRST_Y):
            own2(FIRST_Z[1])
        z_events(s)
        if ended + 1 <= (2 * n) // 3 - 1:
            y_end(FIRST_Y[ended])
            ended += 1
    for s in FIRST_Z:
        y_end(FIRST_Y[ended])
        ended += 1
        z_events(s)
    while ended < len(FIRST_Y):
        y_end(FIRST_Y[ended])
        ended += 1

    for s in SUBS:
        if s.two:
            for q in range(4):
                got(W(s, slice(None), absolute(y_order[3 - q]), 1 - c), dr_sem.at[s.k, q])
                pair_go(s, q).wait_send()
            y_go(s, 0, z).wait_send()
        else:
            got(W(s, y, slice(None), 1 - c), dr_sem.at[s.k, 0])
            core_go(s, 0, y).wait_send()
            if s is FIRST_Y[-1]:
                for q in range(4):
                    got(W(s, 1 - y, absolute(y_order[3 - q]), 1 - c), dr_sem.at[s.k, 1 + q])
                    last_go(s, q).wait_send()
            else:
                got(W(s, 1 - y, slice(None), 1 - c), dr_sem.at[s.k, 1])
                core_go(s, 1, 1 - y).wait_send()
            for n in range(4):
                y_go(s, n, z).wait_send()
        z_go(s, 0, z, away).wait_send()

        @pl.when(inner)
        def _():
            for n in range(1, 5):
                z_go(s, n, z, away).wait_send()


def flush(copies, sem):
    copies = [pltpu.make_async_copy(src, dst, sem.at[n]) for n, (src, dst) in enumerate(copies)]
    for copy in copies:
        copy.start()
    for copy in copies:
        copy.wait()


def write_w(WG0, WG1, WU0, WU1, WB0, WB1, gate, up, down, sem):
    pairs = ((WG0, WG1), gate), ((WU0, WU1), up), ((WB0, WB1), down)
    flush([(pair[l].at[yy], dst.at[l, yy]) for pair, dst in pairs for l in range(L) for yy in range(NY)], sem)


def write_state(MA, MB, VA, VB, *refs):
    pairs = zip((MA.at[0], MA.at[1], MB, VA.at[0], VA.at[1], VB), refs[:6], strict=True)
    flush(list(pairs), refs[6])


def solution(mesh):
    nh = len([s for s in FIRST_Y if s.kind == "B"])
    hbm = pl.BlockSpec(memory_space=pltpu.MemorySpace.HBM)
    vmem = pl.BlockSpec(memory_space=pltpu.MemorySpace.VMEM)
    held = [
        *[((NY, NZ, NC, RA, FF), BF16)] * 4,
        *[((NY, NZ, NC, RB, D), BF16)] * 2,
        ((2, L, RA, FF), F32),
        ((L, RB, D), F32),
        ((2, L, RA, FF), F32),
        ((L, RB, D), F32),
    ]

    def step(*arrays):
        terms, weights, m, v = (arrays[i : i + 3] for i in (0, 3, 6, 9))

        def split(x):
            rows = x.shape[-2] // 16
            return x.reshape(L, NY, NZ, NC, rows, x.shape[-1])

        kept = pl.pallas_call(
            body,
            name="step",
            out_shape=[pltpu.VMEM(shape, dtype) for shape, dtype in held],
            in_specs=[hbm] * 12,
            out_specs=[vmem] * 10,
            scratch_shapes=[
                pltpu.VMEM((8, NZ, RA, CA), BF16),
                pltpu.VMEM((nh, NZ, HB, D), BF16),
                pltpu.VMEM((2, HB, D), BF16),
                pltpu.VMEM((8, 2, 3, RA, CA), BF16),
                pltpu.VMEM((nh, 2, 3, HB, D), BF16),
                pltpu.VMEM((2, 2, 3, NY, HB, D), BF16),
                pltpu.VMEM((8, RA, CA), BF16),
                pltpu.VMEM((4, HB, D), BF16),
                pltpu.VMEM((2, L, RA, FF), BF16),
                pltpu.VMEM((L, RB, D), BF16),
                pltpu.VMEM((16, 8, 128), F32),
                pltpu.SemaphoreType.DMA((NS,)),
                pltpu.SemaphoreType.DMA((9,)),
                pltpu.SemaphoreType.DMA((NS, 5)),
                pltpu.SemaphoreType.DMA((NS, 5)),
                pltpu.SemaphoreType.DMA((NS, 4)),
                pltpu.SemaphoreType.DMA((NS, 4)),
                pltpu.SemaphoreType.DMA((NS, 5)),
                pltpu.SemaphoreType.DMA((NS, 6)),
                pltpu.SemaphoreType.DMA((15,)),
                pltpu.SemaphoreType.DMA((16,)),
            ],
            compiler_params=pltpu.CompilerParams(collective_id=0, has_side_effects=True, vmem_limit_bytes=24 * 2**20),
        )(*(split(t[0]) for t in terms), *(split(w) for w in weights), *m, *v)

        whole = pl.pallas_call(
            write_w,
            name="write_w",
            out_shape=[jax.ShapeDtypeStruct((L, NY, NZ, NC, RA, FF), BF16)] * 2
            + [jax.ShapeDtypeStruct((L, NY, NZ, NC, RB, D), BF16)],
            in_specs=[vmem] * 6,
            out_specs=[hbm] * 3,
            scratch_shapes=[pltpu.SemaphoreType.DMA((12,))],
            compiler_params=pltpu.CompilerParams(vmem_limit_bytes=24 * 2**20),
        )(*kept[:6])
        state = pl.pallas_call(
            write_state,
            name="write_state",
            out_shape=([jax.ShapeDtypeStruct((L, RA, FF), F32)] * 2 + [jax.ShapeDtypeStruct((L, RB, D), F32)]) * 2,
            in_specs=[vmem] * 4,
            out_specs=[hbm] * 6,
            scratch_shapes=[pltpu.SemaphoreType.DMA((6,))],
            compiler_params=pltpu.CompilerParams(vmem_limit_bytes=24 * 2**20),
        )(*kept[6:])
        outs = [*whole, *state]
        whole = [x.reshape(L, -1, x.shape[-1]) for x in outs[:3]]
        return (*whole, *outs[3:])

    all_of, cut = P(None, None, None), P(None, "dp", None)
    return jax.shard_map(
        step,
        mesh=mesh,
        in_specs=(P(("rep", "dp"), None, None, None),) * 3 + (all_of,) * 3 + (cut,) * 6,
        out_specs=(P("rep", None, None),) * 3 + (P("rep", "dp", None),) * 6,
        check_vma=False,
    )
```
